256 devices in a mesh: blk: 16 (over x, y_hi, core), grp: 16 (over y_lo, z).
Axes of the slice: x: 4, y: 4 (y_hi: 2, y_lo: 2; y = y_hi * 2 + y_lo), z: 8, core: 2. Of those that a mesh axis runs over, the one named last changes fastest.
Arguments:
- amplitudes: bfloat16 [896, 4, 896], P('blk', None, 'grp'), may hold values from -6 to 6
- grid_factor: bfloat16 [8192, 896], P(('blk', 'grp')), may hold values from -0.1875 to 0.1875
- metric: float32 [8192, 16, 512], P('blk', 'grp'), may hold values from -0.625 to 0.625
- virt_energy: float32 [896], replicated, may hold values from 0.2 to 4
- pair_energy: float32 [4], replicated, may hold values from -2 to -0.5
Outputs:
- residual: float32 [896, 4, 896], P('blk', None, 'grp')
The draws below stay inside these ranges and needn't reach their ends.
All inputs are finite; a program needn't handle non-finite values.
Results may differ from the reference program's by a relative error of at most 0.005.
Values may be sent and summed in bfloat16 or wider, within the bound.
No kernel may reach another device: no remote copies, remote signals or barrier semaphores. Data moves between devices by JAX's collectives and lax.ppermute only.
A program may use at most 64 MiB of HBM per device.

```python
import math
import jax
import jax.numpy as jnp
from jax import lax

NV = 896
PTS = 32
OP = 4
NG = 8192
N_BLK = 16
N_GRP = 16


def block_levels(stream_key, extent, pieces, least, top_value):
    gain = 1.0
    for position, blocks in pieces:
        heights = jax.random.uniform(jax.random.fold_in(jax.random.fold_in(stream_key, 6), position), (blocks,), jnp.float32, least / len(pieces), top_value / len(pieces))
        gain = gain * jnp.repeat(jnp.exp(heights), extent[position] // blocks).reshape((-1,) + (1,) * (len(extent) - 1 - position))
    return gain


def normal_values(stream_key, extent, width, most, cuts=(), kind=jnp.bfloat16):
    result = jax.random.normal(stream_key, extent, jnp.float32) * width
    if len(cuts) > 0:
        result = block_levels(stream_key, extent, cuts, -0.22, 0.18) * result
    return jnp.clip(result, min=-most, max=most).astype(kind)


def setup_inputs(seed: int = 0) -> dict:
    key_list = jax.random.split(jax.random.key(seed), 6)
    return {
        "amplitudes": normal_values(key_list[0], (NV, OP, NV), 1.0, 6.0, ((0, 16), (2, 16))),
        "grid_factor": normal_values(key_list[1], (NG, NV), NV ** -0.5, 0.1875, ((0, 256),)),
        "metric": normal_values(key_list[2], (NG, N_GRP, N_BLK * PTS), ((NG // NV) ** 2) ** -0.5, 0.625, ((0, 16), (1, 16)), jnp.float32),
        "virt_energy": jnp.clip(jnp.exp(jax.random.uniform(key_list[3], (NV,), jnp.float32, math.log(0.2), math.log(4.0))), 0.2, 4.0),
        "pair_energy": jnp.clip(jax.random.uniform(key_list[4], (OP,), jnp.float32, -2.0, -0.5), -2.0, -0.5),
    }


def reference(amplitudes, grid_factor, metric, virt_energy, pair_energy):
    metric_full = jnp.transpose(metric.reshape(NG, N_GRP, N_BLK, PTS), (0, 2, 1, 3)).reshape(NG, NG)
    factor_split = grid_factor.reshape(N_BLK, N_GRP, PTS, NV)

    def one_pair(pair_amp):
        left = jnp.dot(grid_factor, pair_amp, preferred_element_type=jnp.float32).astype(jnp.bfloat16)
        products = jnp.dot(left, grid_factor.T, preferred_element_type=jnp.float32)
        weighted = (metric_full * products).astype(jnp.bfloat16).reshape(NG, N_BLK, N_GRP, PTS)

        def add_group(summed, group):
            block = lax.dynamic_index_in_dim(weighted, group, 2, keepdims=False).astype(jnp.float32)
            rows = lax.dynamic_index_in_dim(factor_split, group, 1, keepdims=False).astype(jnp.float32)
            partial_sum = jnp.einsum("pbr,brv->pv", block, rows, precision=lax.Precision.HIGHEST)
            rounded = lax.optimization_barrier(partial_sum.astype(jnp.bfloat16))
            return summed + rounded.astype(jnp.float32), None

        summed, unused = lax.scan(add_group, jnp.zeros((NG, NV), jnp.float32), jnp.arange(N_GRP, dtype=jnp.int32))
        mixed = summed.astype(jnp.bfloat16)
        return jnp.dot(grid_factor.T, mixed, preferred_element_type=jnp.float32)

    ladder = lax.map(one_pair, jnp.transpose(amplitudes, (1, 0, 2)))
    ladder = jnp.transpose(ladder, (1, 0, 2))
    denominator = virt_energy[:, None, None] + virt_energy[None, None, :] - pair_energy[None, :, None]
    return denominator * amplitudes.astype(jnp.float32) + ladder
```

```python
import jax
import jax.numpy as jnp
from jax import lax
from jax.sharding import Mesh
from jax.sharding import PartitionSpec as P

BLK = ("x", "y_hi", "core")
GRP = ("y_lo", "z")
PLANE = ("x", "y_hi")
CHUNKS = 2
BF16 = jnp.bfloat16
F32 = jnp.float32


def from_everyone(x, axis):
    count = lax.axis_size(axis)
    return lax.all_to_all(jnp.broadcast_to(x[None], (count, *x.shape)), axis, 0, 0, tiled=True)


def exchanged(x):
    return lax.ppermute(x, "core", [(0, 1), (1, 0)])


def both_cores(own):
    other = exchanged(own)
    first = lax.axis_index("core") == 0
    return jnp.stack([jnp.where(first, own, other), jnp.where(first, other, own)], axis=1)


def local(amplitudes, grid_factor, metric, virt_energy, pair_energy):
    n_c, n_k, n_d = amplitudes.shape
    nv = grid_factor.shape[1]
    n_blk, n_grp = lax.axis_size(BLK), lax.axis_size(GRP)
    turned = amplitudes.transpose(2, 1, 0).reshape(n_d, n_k * n_c)
    turned = from_everyone(turned, GRP).reshape(nv, n_k * n_c)
    columns = both_cores(from_everyone(grid_factor, PLANE)).reshape(-1, nv)
    rows = from_everyone(grid_factor, GRP).reshape(-1, nv)
    n_q = columns.shape[0]
    n_p = rows.shape[0]
    z = metric.reshape(n_p, 1, n_q)
    right = lax.dot_general(
        turned, columns, (((0,), (1,)), ((), ())), preferred_element_type=F32
    ).astype(BF16)
    per = n_k // CHUNKS
    right = right.reshape(CHUNKS, per, n_c, n_q).transpose(0, 2, 1, 3).reshape(CHUNKS, n_c, per * n_q)
    parts = []
    for h in range(CHUNKS):
        full = both_cores(from_everyone(right[h], PLANE)).reshape(nv, per * n_q)
        products = jnp.dot(rows, full, preferred_element_type=F32)
        weighted = (products.reshape(n_p, per, n_q) * z).astype(BF16).reshape(n_p, per * n_q)
        back = lax.dot_general(
            rows, weighted, (((0,), (0,)), ((), ())), preferred_element_type=F32
        ).astype(BF16)
        back = back.reshape(n_blk // 2, 2, n_c, per * n_q)
        first = lax.axis_index("core") == 0
        keep = jnp.where(first, back[:, 0], back[:, 1])
        give = jnp.where(first, back[:, 1], back[:, 0])
        chip = (keep.astype(F32) + exchanged(give).astype(F32)).astype(BF16)
        arrived = lax.all_to_all(chip, PLANE, 0, 0, tiled=True)
        summed = arrived.astype(F32).sum(axis=0).astype(BF16)
        summed = summed.reshape(n_c, per, n_q).transpose(1, 0, 2).reshape(per * n_c, n_q)
        parts.append(
            lax.dot_general(
                columns, summed, (((0,), (1,)), ((), ())), preferred_element_type=F32
            ).astype(BF16)
        )
    ladder = jnp.concatenate(parts, axis=1).reshape(n_grp, n_d, n_k * n_c)
    ladder = lax.all_to_all(ladder, GRP, 0, 0, tiled=True).astype(F32).sum(axis=0)
    ladder = ladder.reshape(n_d, n_k, n_c).transpose(2, 1, 0)
    first_energy = lax.dynamic_slice_in_dim(virt_energy, lax.axis_index(BLK) * n_c, n_c)
    second_energy = lax.dynamic_slice_in_dim(virt_energy, lax.axis_index(GRP) * n_d, n_d)
    denominator = (
        first_energy[:, None, None] + second_energy[None, None, :] - pair_energy[None, :, None]
    )
    return denominator * amplitudes.astype(F32) + ladder


def solution(mesh):
    split = Mesh(mesh.devices.reshape(4, 2, 2, 2, 8), ("x", "y_hi", "core", "y_lo", "z"))
    in_specs = (P(BLK, None, GRP), P(BLK + GRP, None), P(BLK, GRP, None), P(), P())
    return jax.shard_map(
        local, mesh=split, in_specs=in_specs, out_specs=P(BLK, None, GRP), check_vma=False
    )
```

```python
import jax
import jax.numpy as jnp
from jax import lax
from jax.sharding import Mesh
from jax.sharding import PartitionSpec as P
from jax.experimental import pallas as pl
from jax.experimental.pallas import tpu as pltpu

BLK = ("x", "y_hi", "core")
GRP = ("y_lo", "z")
PLANE = ("x", "y_hi")
BF16 = jnp.bfloat16
F32 = jnp.float32


def from_everyone(x, axis):
    count = lax.axis_size(axis)
    return lax.all_to_all(jnp.broadcast_to(x[None], (count, *x.shape)), axis, 0, 0, tiled=True)


def from_ahead(x, axis, offset):
    n = lax.axis_size(axis)
    return lax.ppermute(x, axis, [((i + offset) % n, i) for i in range(n)])


def steps_along(x, axis, order=None):
    n = lax.axis_size(axis)
    arrived = {o: from_ahead(x, axis, o) for o in (order or range(1, n))}
    return jnp.concatenate([x] + [arrived[o] for o in range(1, n)], axis=0)


def kernel_call(body, outs, args, flops=0, scratch=()):
    smem = pl.BlockSpec(memory_space=pltpu.SMEM)
    vmem = pl.BlockSpec(memory_space=pltpu.VMEM)
    moved = sum(a.size * a.dtype.itemsize for a in (*args, *outs))
    return pl.pallas_call(
        body,
        out_shape=outs,
        in_specs=[smem] + [vmem] * (len(args) - 1),
        out_specs=[vmem] * len(outs),
        scratch_shapes=list(scratch),
        cost_estimate=pl.CostEstimate(flops=flops, bytes_accessed=moved, transcendentals=0),
        compiler_params=pltpu.CompilerParams(vmem_limit_bytes=40 * 2**20),
    )(*args)


def placed_by_block(place, pieces, n_x, n_h):
    count = len(pieces)

    def body(place, *refs):
        out = refs[-1]
        for i in range(count):
            core, ox = i // n_x, i % n_x
            for oh in range(n_h):
                b = (
                    ((place[0] + ox) % n_x) * (2 * n_h)
                    + ((place[1] + oh) % n_h) * 2
                    + (place[2] + core) % 2
                )
                out[b] = refs[i][oh]

    shape = (count * n_h, *pieces[0].shape[1:])
    return kernel_call(body, [jax.ShapeDtypeStruct(shape, BF16)], [place, *pieces])[0]


def both_ways(pieces, place):
    n_l, pts, nv = pieces[0].shape
    rows = n_l * pts
    total = rows * len(pieces)

    def body(place, *refs):
        out, turned = refs[-2:]
        for i in range(0, len(pieces), 2):
            block = jnp.concatenate(
                [refs[i + j][...].reshape(rows, nv) for j in range(2)], axis=0
            )
            out[i * rows : (i + 2) * rows, :] = block
            turned[:, i * rows : (i + 2) * rows] = block.T

    outs = [jax.ShapeDtypeStruct((total, nv), BF16), jax.ShapeDtypeStruct((nv, total), BF16)]
    return kernel_call(body, outs, [place, *pieces])


def weighed(place, rows, turned, right, z_own, z_other, half, n_z, n_l):
    total, nv = rows.shape
    n_q = z_own.shape[1]
    pts = total // (2 * n_z * n_l)

    def body(place, rows, turned, right, z_own, z_other, out, weighted):
        for k in range(half):
            cols = slice(k * n_q, (k + 1) * n_q)
            for core, z in enumerate((z_own, z_other)):
                base = core * n_z * n_l * pts
                products = jnp.dot(
                    rows[base : base + n_z * n_l * pts, :],
                    right[:, cols],
                    preferred_element_type=F32,
                )
                for s in range(n_z * n_l):
                    oz, ol = s // n_l, s % n_l
                    g = ((place[1] + ol) % n_l) * n_z + (place[0] + oz) % n_z
                    zs = z[pl.ds(pl.multiple_of(g * pts, pts), pts), :]
                    weighted[base + s * pts : base + (s + 1) * pts, :] = (
                        zs * products[s * pts : (s + 1) * pts, :]
                    ).astype(BF16)
            out[:, cols] = jnp.dot(
                turned[...], weighted[...], preferred_element_type=F32
            ).astype(BF16)

    outs = [jax.ShapeDtypeStruct((nv, half * n_q), BF16)]
    flops = 4 * total * nv * half * n_q
    return kernel_call(
        body,
        outs,
        [place, rows, turned, right, z_own, z_other],
        flops,
        [pltpu.VMEM((total, n_q), BF16)],
    )[0]


def contract_last(a, b):
    return lax.dot_general(a, b, (((0,), (1,)), ((), ())), preferred_element_type=F32)


def in_core_order(own, other, axis):
    first = lax.axis_index("core") == 0
    return jnp.stack([jnp.where(first, own, other), jnp.where(first, other, own)], axis=axis)


def local(amplitudes, grid_factor, metric, virt_energy, pair_energy):
    n_c, n_k, n_d = amplitudes.shape
    _, nv = grid_factor.shape
    n_x, n_h = lax.axis_size("x"), lax.axis_size("y_hi")
    n_z, n_l = lax.axis_size("z"), lax.axis_size("y_lo")
    n_plane, n_grp = n_x * n_h, n_z * n_l
    my_x, my_h, my_core = lax.axis_index("x"), lax.axis_index("y_hi"), lax.axis_index("core")
    my_z, my_l = lax.axis_index("z"), lax.axis_index("y_lo")
    half = n_k // 2
    first = my_core == 0

    turned = amplitudes.transpose(2, 1, 0)
    low = turned[:, :half].reshape(n_d, half * n_c)
    high = turned[:, half:].reshape(n_d, half * n_c)
    other = from_ahead(jnp.where(first, high, low), "core", 1).reshape(n_d, half, n_c)
    own = jnp.where(first, low, high).reshape(n_d, half, n_c)
    turned = in_core_order(own, other, 2).reshape(n_d, half * 2 * n_c)
    turned = from_everyone(turned, GRP).reshape(nv, half * 2 * n_c)

    mine = steps_along(grid_factor[None], "y_hi")
    own = [mine] + [from_ahead(mine, "x", o) for o in range(1, n_x)]
    own += [from_ahead(piece, "core", 1) for piece in own]
    columns = placed_by_block(jnp.stack([my_x, my_h, my_core]), own, n_x, n_h).reshape(-1, nv)
    n_q = columns.shape[0]

    right = contract_last(turned, columns).astype(BF16)
    right = right.reshape(half, 2 * n_c, n_q).transpose(1, 0, 2).reshape(2 * n_c, half * n_q)
    right = from_everyone(right, PLANE).reshape(nv, half * n_q)

    pair = steps_along(grid_factor[None], "y_lo")
    own = {0: pair}
    up = down = pair
    for o in range(1, n_z // 2 + 1):
        up = from_ahead(up, "z", 1)
        if o < n_z - o:
            down = from_ahead(down, "z", -1)
            up, down = lax.optimization_barrier((up, down))
            own[n_z - o] = down
        own[o] = up
    own = [own[o] for o in range(n_z)]
    own += [from_ahead(piece, "core", 1) for piece in own]
    place = jnp.stack([my_z, my_l])
    rows, rows_turned = both_ways(own, place)
    z = metric.reshape(-1, n_q)
    z_other = from_ahead(z, "core", 1)
    back = weighed(place, rows, rows_turned, right, z, z_other, half, n_z, n_l)
    back = back.reshape(n_plane, 2 * n_c, half * n_q)
    back = lax.all_to_all(back, PLANE, 0, 0, tiled=True)
    back = back.astype(F32).sum(axis=0).astype(BF16)
    back = back.reshape(2 * n_c, half, n_q).transpose(1, 0, 2).reshape(half * 2 * n_c, n_q)
    ladder = contract_last(columns, back).astype(BF16).reshape(n_grp, n_d, half * 2 * n_c)
    ladder = lax.all_to_all(ladder, GRP, 0, 0, tiled=True)
    ladder = ladder.astype(F32).sum(axis=0).reshape(n_d, half, 2, n_c)
    keep = jnp.where(first, ladder[:, :, 0], ladder[:, :, 1])
    give = jnp.where(first, ladder[:, :, 1], ladder[:, :, 0])
    other = from_ahead(give.reshape(n_d, half * n_c), "core", 1).reshape(n_d, half, n_c)
    ladder = in_core_order(keep, other, 1).reshape(n_d, n_k, n_c).transpose(2, 1, 0)
    first_energy = lax.dynamic_slice_in_dim(virt_energy, lax.axis_index(BLK) * n_c, n_c)
    second_energy = lax.dynamic_slice_in_dim(virt_energy, lax.axis_index(GRP) * n_d, n_d)
    denominator = (
        first_energy[:, None, None] + second_energy[None, None, :] - pair_energy[None, :, None]
    )
    return denominator * amplitudes.astype(F32) + ladder


def solution(mesh):
    split = Mesh(mesh.devices.reshape(4, 2, 2, 2, 8), ("x", "y_hi", "core", "y_lo", "z"))
    in_specs = (P(BLK, None, GRP), P(BLK + GRP, None), P(BLK, GRP, None), P(), P())
    return jax.shard_map(
        local, mesh=split, in_specs=in_specs, out_specs=P(BLK, None, GRP), check_vma=False
    )
```

```python
import jax
import jax.numpy as jnp
from jax import lax
from jax.sharding import Mesh
from jax.sharding import PartitionSpec as P
from jax.experimental import pallas as pl
from jax.experimental.pallas import tpu as pltpu

BLK = ("x", "y_hi", "core")
GRP = ("y_lo", "z")
BF16 = jnp.bfloat16
F32 = jnp.float32


def from_ahead(x, axis, offset):
    n = lax.axis_size(axis)
    return lax.ppermute(x, axis, [((i + offset) % n, i) for i in range(n)])


def to_ahead(x, axis, offset):
    n = lax.axis_size(axis)
    return lax.ppermute(x, axis, [(i, (i + offset) % n) for i in range(n)])


def total(parts):
    return sum(p.astype(F32) for p in parts).astype(BF16)


def steps_along(x, axis, order=None):
    n = lax.axis_size(axis)
    arrived = {o: from_ahead(x, axis, o) for o in (order or range(1, n))}
    return jnp.concatenate([x] + [arrived[o] for o in range(1, n)], axis=0)


def kernel_call(body, outs, args, flops=0, scratch=(), far=()):
    smem = pl.BlockSpec(memory_space=pltpu.SMEM)
    vmem = pl.BlockSpec(memory_space=pltpu.VMEM)
    moved = sum(a.size * a.dtype.itemsize for a in (*args, *outs))
    return pl.pallas_call(
        body,
        out_shape=outs,
        in_specs=[smem]
        + [pl.BlockSpec(memory_space=pl.ANY) if i in far else vmem for i in range(1, len(args))],
        out_specs=[vmem] * len(outs),
        scratch_shapes=list(scratch),
        cost_estimate=pl.CostEstimate(flops=flops, bytes_accessed=moved, transcendentals=0),
        compiler_params=pltpu.CompilerParams(vmem_limit_bytes=40 * 2**20),
    )(*args)


def turned_copies(core, own, other, count):
    n_c, n_k, n_d = own.shape
    half = n_k // 2

    def body(core, own, other, out):
        mine = own[...].astype(F32)
        theirs = other[...].astype(F32)
        is_low = core[0] == 0
        blocks = []
        for k in range(half):
            a = jnp.where(is_low, mine[:, k], mine[:, half + k])
            b = jnp.where(is_low, theirs[:, k], theirs[:, half + k])
            blocks += [jnp.where(is_low, a, b), jnp.where(is_low, b, a)]
        whole = jnp.concatenate(blocks, axis=0).T.astype(BF16)
        for i in range(count):
            out[i] = whole

    shape = jax.ShapeDtypeStruct((count, n_d, half * 2 * n_c), BF16)
    return kernel_call(body, [shape], [core, own, other])[0]


def right_of(core, turned, columns, half):
    n_grp, n_d, width = turned.shape
    n_q = columns.shape[0]
    rows = width // half

    def body(core, turned, columns, *outs):
        left = turned[...].reshape(n_grp * n_d, width).T
        right = lax.dot_general(
            left, columns[...], (((1,), (1,)), ((), ())), preferred_element_type=F32
        ).astype(BF16)
        for k in range(half):
            outs[k][...] = right[k * rows : (k + 1) * rows]

    outs = [jax.ShapeDtypeStruct((rows, n_q), BF16)] * half
    return kernel_call(body, outs, [core, turned, columns], 2 * n_q * n_grp * n_d * width)


def placed_by_block(place, pieces, n_x, n_h):
    count = len(pieces)

    def body(place, *refs):
        out = refs[-1]
        for i in range(count):
            core, ox = i // n_x, i % n_x
            for oh in range(n_h):
                b = (
                    ((place[0] + ox) % n_x) * (2 * n_h)
                    + ((place[1] + oh) % n_h) * 2
                    + (place[2] + core) % 2
                )
                out[b] = refs[i][oh]

    shape = (count * n_h, *pieces[0].shape[1:])
    return kernel_call(body, [jax.ShapeDtypeStruct(shape, BF16)], [place, *pieces])[0]


def weighed(place, pieces, right, z_own, z_other, half, n_z, n_l, n_x, n_h):
    pts, nv = pieces[0].shape[1:]
    step = n_l * pts
    total = step * len(pieces)
    n_q = right[0].shape[2]
    lanes = z_own.shape[1]
    per_row = n_q // lanes
    n_plane = n_x * n_h
    share = nv // n_plane
    count = len(pieces)

    def body(place, *refs):
        parts, rights = refs[:count], refs[count : count + n_x + n_h]
        far_own, far_other = refs[count + n_x + n_h : count + n_x + n_h + 2]
        outs = refs[count + n_x + n_h + 2 : -7]
        rows, turned, weighted, right, z_own, z_other, done = refs[-7:]
        copies = [
            pltpu.make_async_copy(far_own, z_own, done.at[0]),
            pltpu.make_async_copy(far_other, z_other, done.at[1]),
        ]
        for copy in copies:
            copy.start()
        slots = []
        for j in range(n_plane):
            ox = (j // n_h + n_x - place[2]) % n_x
            oh = (j % n_h + n_h - place[3]) % n_h
            slots.append(ox * n_h + oh)
        for i in range(0, count, 2):
            block = jnp.concatenate(
                [parts[i + j][...].reshape(step, nv) for j in range(2)], axis=0
            )
            rows[i * step : (i + 2) * step, :] = block
            flipped = block.T
            for j in range(n_plane):
                turned[slots[j], :, i * step : (i + 2) * step] = flipped[
                    j * share : (j + 1) * share
                ]
        for k in range(half):
            for ox in range(n_x):
                for oh in range(n_h):
                    at = ((place[2] + ox) % n_x) * n_h + (place[3] + oh) % n_h
                    right[at] = rights[ox][oh] if k == 0 else rights[n_x + oh][ox]
            for core, z in enumerate((z_own, z_other)):
                base = core * n_z * step
                products = jnp.dot(
                    rows[base : base + n_z * step, :],
                    right[...].reshape(nv, n_q),
                    preferred_element_type=F32,
                )
                if k == 0:
                    copies[core].wait()
                for s in range(n_z * n_l):
                    oz, ol = s // n_l, s % n_l
                    g = ((place[1] + ol) % n_l) * n_z + (place[0] + oz) % n_z
                    first = g * (pts * per_row)
                    for j in range(per_row):
                        zs = z[pl.ds(first + j, pts, stride=per_row), :]
                        weighted[
                            base + s * pts : base + (s + 1) * pts, j * lanes : (j + 1) * lanes
                        ] = (
                            zs * products[s * pts : (s + 1) * pts, j * lanes : (j + 1) * lanes]
                        ).astype(BF16)
            back = jnp.dot(
                turned[...].reshape(nv, total), weighted[...], preferred_element_type=F32
            ).astype(BF16)
            for ox in range(n_x):
                for oh in range(n_h):
                    at = (ox * n_h + oh) * share
                    block = back[at : at + share]
                    if k == 0:
                        outs[ox][oh] = block
                    else:
                        outs[n_x + oh][ox] = block

    outs = [jax.ShapeDtypeStruct((n_h, share, n_q), BF16)] * n_x
    outs += [jax.ShapeDtypeStruct((n_x, share, n_q), BF16)] * n_h
    flops = 4 * total * nv * half * n_q
    scratch = [
        pltpu.VMEM((total, nv), BF16),
        pltpu.VMEM((n_plane, share, total), BF16),
        pltpu.VMEM((total, n_q), BF16),
        pltpu.VMEM((n_plane, share, n_q), BF16),
        pltpu.VMEM(z_own.shape, F32),
        pltpu.VMEM(z_own.shape, F32),
        pltpu.SemaphoreType.DMA((2,)),
    ]
    args = [place, *pieces, *right, z_own, z_other]
    return kernel_call(body, outs, args, flops, scratch, (len(args) - 2, len(args) - 1))


def contract_last(a, b):
    return lax.dot_general(a, b, (((0,), (1,)), ((), ())), preferred_element_type=F32)


def in_core_order(own, other, axis):
    first = lax.axis_index("core") == 0
    return jnp.stack([jnp.where(first, own, other), jnp.where(first, other, own)], axis=axis)


def local(amplitudes, grid_factor, metric, virt_energy, pair_energy):
    n_c, n_k, n_d = amplitudes.shape
    _, nv = grid_factor.shape
    n_x, n_h = lax.axis_size("x"), lax.axis_size("y_hi")
    n_z, n_l = lax.axis_size("z"), lax.axis_size("y_lo")
    n_grp = n_z * n_l
    half = n_k // 2
    my_x, my_h, my_core = lax.axis_index("x"), lax.axis_index("y_hi"), lax.axis_index("core")
    my_z, my_l = lax.axis_index("z"), lax.axis_index("y_lo")
    half = n_k // 2
    first = my_core == 0

    other = from_ahead(amplitudes, "core", 1)
    turned = turned_copies(my_core[None], amplitudes, other, n_z * n_l)
    turned = lax.all_to_all(turned, GRP, 0, 0, tiled=True)

    mine = steps_along(grid_factor[None], "y_hi")
    own = [mine] + [from_ahead(mine, "x", o) for o in range(1, n_x)]
    own += [from_ahead(piece, "core", 1) for piece in own]
    columns = placed_by_block(jnp.stack([my_x, my_h, my_core]), own, n_x, n_h).reshape(-1, nv)

    right = right_of(my_core[None], turned, columns, half)
    low = from_ahead(right[0], "y_hi", 1)
    high = [right[1]] + [from_ahead(right[1], "x", o) for o in (1, 3, 2)]
    low = jnp.stack([right[0], low])
    high = jnp.stack([high[o] for o in (0, 1, 3, 2)])
    low = {0: low, **{o: from_ahead(low, "x", o) for o in (1, 3, 2)}}
    right = [low[o] for o in range(n_x)] + [high, from_ahead(high, "y_hi", 1)]

    pair = steps_along(grid_factor[None], "y_lo")
    own = {0: pair}
    up = down = pair
    for o in range(1, n_z // 2 + 1):
        up = from_ahead(up, "z", 1)
        if o < n_z - o:
            down = from_ahead(down, "z", -1)
            up, down = lax.optimization_barrier((up, down))
            own[n_z - o] = down
        own[o] = up
    own = [own[o] for o in range(n_z)]
    own += [from_ahead(piece, "core", 1) for piece in own]
    z = metric.reshape(-1, 128)
    z_other = from_ahead(z, "core", 1)
    place = jnp.stack([my_z, my_l, my_x, my_h])
    sums = weighed(place, own, right, z, z_other, half, n_z, n_l, n_x, n_h)
    low, high = sums[:n_x], sums[n_x:]
    high_arrived = to_ahead(high[1], "y_hi", 1)
    low_arrived = [to_ahead(low[o], "x", o) for o in (1, 3, 2)]
    low = [total([low[0][h]] + [p[h] for p in low_arrived]) for h in range(n_h)]
    high = [total([high[0][o], high_arrived[o]]) for o in range(n_x)]
    low_arrived = to_ahead(low[1], "y_hi", 1)
    high_arrived = [to_ahead(high[o], "x", o) for o in (1, 3, 2)]
    back = jnp.concatenate([total([low[0], low_arrived]), total([high[0]] + high_arrived)], axis=0)
    ladder = contract_last(columns, back).astype(BF16).reshape(n_grp, n_d, half * 2 * n_c)
    ladder = lax.all_to_all(ladder, GRP, 0, 0, tiled=True)
    ladder = ladder.astype(F32).sum(axis=0).reshape(n_d, half, 2, n_c)
    keep = jnp.where(first, ladder[:, :, 0], ladder[:, :, 1])
    give = jnp.where(first, ladder[:, :, 1], ladder[:, :, 0])
    other = from_ahead(give.reshape(n_d, half * n_c), "core", 1).reshape(n_d, half, n_c)
    ladder = in_core_order(keep, other, 1).reshape(n_d, n_k, n_c).transpose(2, 1, 0)
    first_energy = lax.dynamic_slice_in_dim(virt_energy, lax.axis_index(BLK) * n_c, n_c)
    second_energy = lax.dynamic_slice_in_dim(virt_energy, lax.axis_index(GRP) * n_d, n_d)
    denominator = (
        first_energy[:, None, None] + second_energy[None, None, :] - pair_energy[None, :, None]
    )
    return denominator * amplitudes.astype(F32) + ladder


def solution(mesh):
    split = Mesh(mesh.devices.reshape(4, 2, 2, 2, 8), ("x", "y_hi", "core", "y_lo", "z"))
    in_specs = (P(BLK, None, GRP), P(BLK + GRP, None), P(BLK, GRP, None), P(), P())
    return jax.shard_map(
        local, mesh=split, in_specs=in_specs, out_specs=P(BLK, None, GRP), check_vma=False
    )
```

```python
import jax
import jax.numpy as jnp
from jax import lax
from jax.sharding import Mesh
from jax.sharding import PartitionSpec as P
from jax.experimental import pallas as pl
from jax.experimental.pallas import tpu as pltpu

BLK = ("x", "y_hi", "core")
GRP = ("y_lo", "z")
BF16 = jnp.bfloat16
F32 = jnp.float32
FIRST_PART = 640


def from_ahead(x, axis, offset):
    n = lax.axis_size(axis)
    return lax.ppermute(x, axis, [((i + offset) % n, i) for i in range(n)])


def to_ahead(x, axis, offset):
    n = lax.axis_size(axis)
    return lax.ppermute(x, axis, [(i, (i + offset) % n) for i in range(n)])


def total(parts):
    return sum(p.astype(F32) for p in parts).astype(BF16)


def steps_along(x, axis, order=None):
    n = lax.axis_size(axis)
    arrived = {o: from_ahead(x, axis, o) for o in (order or range(1, n))}
    return jnp.concatenate([x] + [arrived[o] for o in range(1, n)], axis=0)


def kernel_call(body, outs, args, flops=0, scratch=(), far=()):
    smem = pl.BlockSpec(memory_space=pltpu.SMEM)
    vmem = pl.BlockSpec(memory_space=pltpu.VMEM)
    moved = sum(a.size * a.dtype.itemsize for a in (*args, *outs))
    return pl.pallas_call(
        body,
        out_shape=outs,
        in_specs=[smem]
        + [pl.BlockSpec(memory_space=pl.ANY) if i in far else vmem for i in range(1, len(args))],
        out_specs=[vmem] * len(outs),
        scratch_shapes=list(scratch),
        cost_estimate=pl.CostEstimate(flops=flops, bytes_accessed=moved, transcendentals=0),
        compiler_params=pltpu.CompilerParams(vmem_limit_bytes=40 * 2**20),
    )(*args)


def turned_copies(core, own, other, count):
    n_c, n_k, n_d = own.shape
    half = n_k // 2

    def body(core, own, other, out):
        mine = own[...].astype(F32)
        theirs = other[...].astype(F32)
        is_low = core[0] == 0
        blocks = []
        for k in range(half):
            a = jnp.where(is_low, mine[:, k], mine[:, half + k])
            b = jnp.where(is_low, theirs[:, k], theirs[:, half + k])
            blocks += [jnp.where(is_low, a, b), jnp.where(is_low, b, a)]
        whole = jnp.concatenate(blocks, axis=0).T.astype(BF16)
        for i in range(count):
            out[i] = whole

    shape = jax.ShapeDtypeStruct((count, n_d, half * 2 * n_c), BF16)
    return kernel_call(body, [shape], [core, own, other])[0]


def right_of(core, turned, columns, half, first_part):
    n_grp, n_d, width = turned.shape
    n_q = columns.shape[0]
    rows = width // half

    def body(core, turned, columns, *outs):
        left = turned[...].reshape(n_grp * n_d, width).T
        right = lax.dot_general(
            left, columns[...], (((1,), (1,)), ((), ())), preferred_element_type=F32
        ).astype(BF16)
        whole = jnp.concatenate([right[k * rows : (k + 1) * rows] for k in range(half)], axis=1)
        outs[0][...] = whole[:, :first_part]
        outs[1][...] = whole[:, first_part:]

    widths = (first_part, half * n_q - first_part)
    outs = [jax.ShapeDtypeStruct((rows, w), BF16) for w in widths]
    return kernel_call(body, outs, [core, turned, columns], 2 * n_q * n_grp * n_d * width)


def ladder_of(core, parts, columns, n_grp):
    n_q, nv = columns.shape
    rows = parts[0][0].shape[0]
    half = len(parts)
    count = [len(p) for p in parts]

    def body(core, *refs):
        columns, out = refs[-2:]
        at, sums = 0, []
        for n in count:
            sums.append(sum(r[...].astype(F32) for r in refs[at : at + n]).astype(BF16))
            at += n
        whole = jnp.dot(
            jnp.concatenate(sums, axis=0), columns[...], preferred_element_type=F32
        )
        out[...] = whole.T.astype(BF16).reshape(n_grp, nv // n_grp, half * rows)

    shape = jax.ShapeDtypeStruct((n_grp, nv // n_grp, half * rows), BF16)
    args = [core, *[x for p in parts for x in p], columns]
    return kernel_call(body, [shape], args, 2 * n_q * nv * half * rows)[0]


def placed_by_block(place, pieces, n_x, n_h):
    count = len(pieces)

    def body(place, *refs):
        out = refs[-1]
        for i in range(count):
            core, ox = i // n_x, i % n_x
            for oh in range(n_h):
                b = (
                    ((place[0] + ox) % n_x) * (2 * n_h)
                    + ((place[1] + oh) % n_h) * 2
                    + (place[2] + core) % 2
                )
                out[b] = refs[i][oh]

    shape = (count * n_h, *pieces[0].shape[1:])
    return kernel_call(body, [jax.ShapeDtypeStruct(shape, BF16)], [place, *pieces])[0]


def weighed(place, pieces, right, z_own, z_other, half, n_z, n_l, n_x, n_h):
    pts, nv = pieces[0].shape[1:]
    step = n_l * pts
    total = step * len(pieces)
    n_q = (right[0].shape[2] + right[-1].shape[2]) // half
    cut = right[0].shape[2]
    lanes = z_own.shape[1]
    per_row = n_q // lanes
    n_plane = n_x * n_h
    share = nv // n_plane
    count = len(pieces)

    def body(place, *refs):
        parts, rights = refs[:count], refs[count : count + n_x + n_h]
        far_own, far_other = refs[count + n_x + n_h : count + n_x + n_h + 2]
        outs = refs[count + n_x + n_h + 2 : -7]
        rows, turned, weighted, right, z_own, z_other, done = refs[-7:]
        copies = [
            pltpu.make_async_copy(far_own, z_own, done.at[0]),
            pltpu.make_async_copy(far_other, z_other, done.at[1]),
        ]
        for copy in copies:
            copy.start()
        slots = []
        for j in range(n_plane):
            ox = (j // n_h + n_x - place[2]) % n_x
            oh = (j % n_h + n_h - place[3]) % n_h
            slots.append(ox * n_h + oh)
        for i in range(0, count, 2):
            block = jnp.concatenate(
                [parts[i + j][...].reshape(step, nv) for j in range(2)], axis=0
            )
            rows[i * step : (i + 2) * step, :] = block
            flipped = block.T
            for j in range(n_plane):
                turned[slots[j], :, i * step : (i + 2) * step] = flipped[
                    j * share : (j + 1) * share
                ]
        for ox in range(n_x):
            for oh in range(n_h):
                at = ((place[2] + ox) % n_x) * n_h + (place[3] + oh) % n_h
                for k in range(half):
                    low, high = k * n_q, (k + 1) * n_q
                    if low < cut:
                        end = min(high, cut)
                        right[k, at, :, : end - low] = rights[ox][oh, :, low:end]
                    if high > cut:
                        start = max(low, cut)
                        right[k, at, :, start - low :] = rights[n_x + oh][
                            ox, :, start - cut : high - cut
                        ]
        for k in range(half):
            products = jnp.dot(
                rows[...],
                right[k].reshape(nv, n_q),
                preferred_element_type=F32,
            )
            for core, z in enumerate((z_own, z_other)):
                if k == 0:
                    copies[core].wait()
                for s in range(n_z * n_l):
                    oz, ol = s // n_l, s % n_l
                    g = ((place[1] + ol) % n_l) * n_z + (place[0] + oz) % n_z
                    first = g * (pts * per_row)
                    at = core * n_z * step + s * pts
                    for j in range(per_row):
                        zs = z[pl.ds(first + j, pts, stride=per_row), :]
                        cols = slice(j * lanes, (j + 1) * lanes)
                        weighted[at : at + pts, cols] = (
                            zs * products[at : at + pts, cols]
                        ).astype(BF16)
            back = jnp.dot(
                turned[...].reshape(nv, total), weighted[...], preferred_element_type=F32
            ).astype(BF16)
            for ox in range(n_x):
                for oh in range(n_h):
                    at = (ox * n_h + oh) * share
                    block = back[at : at + share]
                    if k == 0:
                        outs[ox][oh] = block
                    else:
                        outs[n_x + oh][ox] = block

    outs = [jax.ShapeDtypeStruct((n_h, share, n_q), BF16)] * n_x
    outs += [jax.ShapeDtypeStruct((n_x, share, n_q), BF16)] * n_h
    flops = 4 * total * nv * half * n_q
    scratch = [
        pltpu.VMEM((total, nv), BF16),
        pltpu.VMEM((n_plane, share, total), BF16),
        pltpu.VMEM((total, n_q), BF16),
        pltpu.VMEM((half, n_plane, share, n_q), BF16),
        pltpu.VMEM(z_own.shape, F32),
        pltpu.VMEM(z_own.shape, F32),
        pltpu.SemaphoreType.DMA((2,)),
    ]
    args = [place, *pieces, *right, z_own, z_other]
    return kernel_call(body, outs, args, flops, scratch, (len(args) - 2, len(args) - 1))


def in_core_order(own, other, axis):
    first = lax.axis_index("core") == 0
    return jnp.stack([jnp.where(first, own, other), jnp.where(first, other, own)], axis=axis)


def local(amplitudes, grid_factor, metric, virt_energy, pair_energy):
    n_c, n_k, n_d = amplitudes.shape
    _, nv = grid_factor.shape
    n_x, n_h = lax.axis_size("x"), lax.axis_size("y_hi")
    n_z, n_l = lax.axis_size("z"), lax.axis_size("y_lo")
    n_grp = n_z * n_l
    half = n_k // 2
    my_x, my_h, my_core = lax.axis_index("x"), lax.axis_index("y_hi"), lax.axis_index("core")
    my_z, my_l = lax.axis_index("z"), lax.axis_index("y_lo")
    half = n_k // 2
    first = my_core == 0

    other = from_ahead(amplitudes, "core", 1)
    turned = turned_copies(my_core[None], amplitudes, other, n_z * n_l)
    turned = lax.all_to_all(turned, GRP, 0, 0, tiled=True)

    mine = steps_along(grid_factor[None], "y_hi")
    own = [mine] + [from_ahead(mine, "x", o) for o in range(1, n_x)]
    own += [from_ahead(piece, "core", 1) for piece in own]
    columns = placed_by_block(jnp.stack([my_x, my_h, my_core]), own, n_x, n_h).reshape(-1, nv)

    right = right_of(my_core[None], turned, columns, half, FIRST_PART)
    low = from_ahead(right[0], "y_hi", 1)
    high = [right[1]] + [from_ahead(right[1], "x", o) for o in (1, 3, 2)]
    low = jnp.stack([right[0], low])
    high = jnp.stack([high[o] for o in (0, 1, 3, 2)])
    low = {0: low, **{o: from_ahead(low, "x", o) for o in (1, 3, 2)}}
    right = [low[o] for o in range(n_x)] + [high, from_ahead(high, "y_hi", 1)]

    pair = steps_along(grid_factor[None], "y_lo")
    own = {0: pair}
    own[1], own[n_z - 1] = from_ahead(pair, "z", 1), from_ahead(pair, "z", -1)
    own[n_z // 2] = from_ahead(pair, "z", n_z // 2)
    for o in range(2, n_z // 2):
        up, down = lax.optimization_barrier((own[o - 1], own[n_z - o + 1]))
        own[o], own[n_z - o] = from_ahead(up, "z", 1), from_ahead(down, "z", -1)
    own = [own[o] for o in range(n_z)]
    others = []
    for o in range(n_z):
        others.append(from_ahead(own[o], "core", 1))
    own += others
    z = metric.reshape(-1, 128)
    z_other = from_ahead(z, "core", 1)
    place = jnp.stack([my_z, my_l, my_x, my_h])
    sums = weighed(place, own, right, z, z_other, half, n_z, n_l, n_x, n_h)
    low, high = sums[:n_x], sums[n_x:]
    high_arrived = to_ahead(high[1], "y_hi", 1)
    low_arrived = [to_ahead(low[o], "x", o) for o in (1, 3, 2)]
    low = [total([low[0][h]] + [p[h] for p in low_arrived]) for h in range(n_h)]
    high = [total([high[0][o], high_arrived[o]]) for o in range(n_x)]
    low_arrived = to_ahead(low[1], "y_hi", 1)
    high_arrived = [to_ahead(high[o], "x", o) for o in (1, 3, 2)]
    parts = [[low[0], low_arrived], [high[0], *high_arrived]]
    ladder = ladder_of(my_core[None], parts, columns, n_grp)
    ladder = lax.all_to_all(ladder, GRP, 0, 0, tiled=True)
    ladder = ladder.astype(F32).sum(axis=0).reshape(n_d, half, 2, n_c)
    keep = jnp.where(first, ladder[:, :, 0], ladder[:, :, 1])
    give = jnp.where(first, ladder[:, :, 1], ladder[:, :, 0])
    other = from_ahead(give.reshape(n_d, half * n_c), "core", 1).reshape(n_d, half, n_c)
    ladder = in_core_order(keep, other, 1).reshape(n_d, n_k, n_c).transpose(2, 1, 0)
    first_energy = lax.dynamic_slice_in_dim(virt_energy, lax.axis_index(BLK) * n_c, n_c)
    second_energy = lax.dynamic_slice_in_dim(virt_energy, lax.axis_index(GRP) * n_d, n_d)
    denominator = (
        first_energy[:, None, None] + second_energy[None, None, :] - pair_energy[None, :, None]
    )
    return denominator * amplitudes.astype(F32) + ladder


def solution(mesh):
    split = Mesh(mesh.devices.reshape(4, 2, 2, 2, 8), ("x", "y_hi", "core", "y_lo", "z"))
    in_specs = (P(BLK, None, GRP), P(BLK + GRP, None), P(BLK, GRP, None), P(), P())
    return jax.shard_map(
        local, mesh=split, in_specs=in_specs, out_specs=P(BLK, None, GRP), check_vma=False
    )
```

```python
import jax
import jax.numpy as jnp
from jax import lax
from jax.sharding import Mesh
from jax.sharding import PartitionSpec as P
from jax.experimental import pallas as pl
from jax.experimental.pallas import tpu as pltpu

BLK = ("x", "y_hi", "core")
GRP = ("y_lo", "z")
BF16 = jnp.bfloat16
F32 = jnp.float32
FIRST_PART = 512


def from_ahead(x, axis, offset):
    n = lax.axis_size(axis)
    return lax.ppermute(x, axis, [((i + offset) % n, i) for i in range(n)])


def to_ahead(x, axis, offset):
    n = lax.axis_size(axis)
    return lax.ppermute(x, axis, [(i, (i + offset) % n) for i in range(n)])


def total(parts):
    return sum(p.astype(F32) for p in parts).astype(BF16)


def steps_along(x, axis, order=None):
    n = lax.axis_size(axis)
    arrived = {o: from_ahead(x, axis, o) for o in (order or range(1, n))}
    return jnp.concatenate([x] + [arrived[o] for o in range(1, n)], axis=0)


def kernel_call(body, outs, args, flops=0, scratch=(), far=()):
    smem = pl.BlockSpec(memory_space=pltpu.SMEM)
    vmem = pl.BlockSpec(memory_space=pltpu.VMEM)
    moved = sum(a.size * a.dtype.itemsize for a in (*args, *outs))
    return pl.pallas_call(
        body,
        out_shape=outs,
        in_specs=[smem]
        + [pl.BlockSpec(memory_space=pl.ANY) if i in far else vmem for i in range(1, len(args))],
        out_specs=[vmem] * len(outs),
        scratch_shapes=list(scratch),
        cost_estimate=pl.CostEstimate(flops=flops, bytes_accessed=moved, transcendentals=0),
        compiler_params=pltpu.CompilerParams(vmem_limit_bytes=40 * 2**20),
    )(*args)


def turned_copies(core, own, other, count):
    n_c, n_k, n_d = own.shape
    half = n_k // 2

    def body(core, own, other, out):
        mine = own[...].astype(F32)
        theirs = other[...].astype(F32)
        is_low = core[0] == 0
        blocks = []
        for k in range(half):
            a = jnp.where(is_low, mine[:, k], mine[:, half + k])
            b = jnp.where(is_low, theirs[:, k], theirs[:, half + k])
            blocks += [jnp.where(is_low, a, b), jnp.where(is_low, b, a)]
        whole = jnp.concatenate(blocks, axis=0).T.astype(BF16)
        for i in range(count):
            out[i] = whole

    shape = jax.ShapeDtypeStruct((count, n_d, half * 2 * n_c), BF16)
    return kernel_call(body, [shape], [core, own, other])[0]


def right_of(core, turned, columns, half, first_part):
    n_grp, n_d, width = turned.shape
    n_q = columns.shape[0]
    rows = width // half

    def body(core, turned, columns, *outs):
        left = turned[...].reshape(n_grp * n_d, width).T
        right = lax.dot_general(
            left, columns[...], (((1,), (1,)), ((), ())), preferred_element_type=F32
        ).astype(BF16)
        whole = jnp.concatenate([right[k * rows : (k + 1) * rows] for k in range(half)], axis=1)
        outs[0][...] = whole[:, :first_part]
        outs[1][...] = whole[:, first_part:]

    widths = (first_part, half * n_q - first_part)
    outs = [jax.ShapeDtypeStruct((rows, w), BF16) for w in widths]
    return kernel_call(body, outs, [core, turned, columns], 2 * n_q * n_grp * n_d * width)


def ladder_of(core, parts, columns, n_grp):
    n_q, nv = columns.shape
    rows = parts[0][0].shape[0]
    half = len(parts)
    count = [len(p) for p in parts]

    def body(core, *refs):
        columns, out = refs[-2:]
        at, sums = 0, []
        for n in count:
            sums.append(sum(r[...].astype(F32) for r in refs[at : at + n]).astype(BF16))
            at += n
        whole = jnp.dot(
            jnp.concatenate(sums, axis=0), columns[...], preferred_element_type=F32
        )
        out[...] = whole.T.astype(BF16).reshape(n_grp, nv // n_grp, half * rows)

    shape = jax.ShapeDtypeStruct((n_grp, nv // n_grp, half * rows), BF16)
    args = [core, *[x for p in parts for x in p], columns]
    return kernel_call(body, [shape], args, 2 * n_q * nv * half * rows)[0]


def placed_by_block(place, pieces, n_x, n_h):
    count = len(pieces)

    def body(place, *refs):
        out = refs[-1]
        for i in range(count):
            core, ox = i // n_x, i % n_x
            for oh in range(n_h):
                b = (
                    ((place[0] + ox) % n_x) * (2 * n_h)
                    + ((place[1] + oh) % n_h) * 2
                    + (place[2] + core) % 2
                )
                out[b] = refs[i][oh]

    shape = (count * n_h, *pieces[0].shape[1:])
    return kernel_call(body, [jax.ShapeDtypeStruct(shape, BF16)], [place, *pieces])[0]


def weighed(place, pieces, right, z_own, z_other, half, n_z, n_l, n_x, n_h):
    keys, pieces = [k for k, _ in pieces], [p for _, p in pieces]
    pts, nv = pieces[0].shape[1:]
    step = n_l * pts
    total = 2 * n_z * step
    n_q = (right[0].shape[2] + right[-1].shape[2]) // half
    cut = right[0].shape[2]
    lanes = z_own.shape[1]
    per_row = n_q // lanes
    n_plane = n_x * n_h
    share = nv // n_plane
    count = len(pieces)

    def body(place, *refs):
        parts, rights = refs[:count], refs[count : count + n_x + n_h]
        far_own, far_other = refs[count + n_x + n_h : count + n_x + n_h + 2]
        outs = refs[count + n_x + n_h + 2 : -7]
        rows, turned, weighted, right, z_own, z_other, done = refs[-7:]
        copies = [
            pltpu.make_async_copy(far_own, z_own, done.at[0]),
            pltpu.make_async_copy(far_other, z_other, done.at[1]),
        ]
        for copy in copies:
            copy.start()
        slots = []
        for j in range(n_plane):
            ox = (j // n_h + n_x - place[2]) % n_x
            oh = (j % n_h + n_h - place[3]) % n_h
            slots.append(ox * n_h + oh)
        offsets = []
        for key, part in zip(keys, parts):
            at = len(offsets) * step
            rows[at : at + len(key) * step, :] = part[...].reshape(len(key) * step, nv)
            offsets += key
        for i in range(0, total, 128):
            flipped = rows[i : i + 128, :].T
            for j in range(n_plane):
                turned[slots[j], :, i : i + 128] = flipped[j * share : (j + 1) * share]
        for ox in range(n_x):
            for oh in range(n_h):
                at = ((place[2] + ox) % n_x) * n_h + (place[3] + oh) % n_h
                for k in range(half):
                    low, high = k * n_q, (k + 1) * n_q
                    if low < cut:
                        end = min(high, cut)
                        right[k, at, :, : end - low] = rights[ox][oh, :, low:end]
                    if high > cut:
                        start = max(low, cut)
                        right[k, at, :, start - low :] = rights[n_x + oh][
                            ox, :, start - cut : high - cut
                        ]
        for k in range(half):
            products = jnp.dot(
                rows[...],
                right[k].reshape(nv, n_q),
                preferred_element_type=F32,
            )
            if k == 0:
                for copy in copies:
                    copy.wait()
            for i, oz in enumerate(offsets):
                z = z_own if i < n_z else z_other
                for ol in range(n_l):
                    g = ((place[1] + ol) % n_l) * n_z + (place[0] + oz) % n_z
                    first = g * (pts * per_row)
                    at = i * step + ol * pts
                    for j in range(per_row):
                        zs = z[pl.ds(first + j, pts, stride=per_row), :]
                        cols = slice(j * lanes, (j + 1) * lanes)
                        weighted[at : at + pts, cols] = (
                            zs * products[at : at + pts, cols]
                        ).astype(BF16)
            back = jnp.dot(
                turned[...].reshape(nv, total), weighted[...], preferred_element_type=F32
            ).astype(BF16)
            for ox in range(n_x):
                for oh in range(n_h):
                    at = (ox * n_h + oh) * share
                    block = back[at : at + share]
                    if k == 0:
                        outs[ox][oh] = block
                    else:
                        outs[n_x + oh][ox] = block

    outs = [jax.ShapeDtypeStruct((n_h, share, n_q), BF16)] * n_x
    outs += [jax.ShapeDtypeStruct((n_x, share, n_q), BF16)] * n_h
    flops = 4 * total * nv * half * n_q
    scratch = [
        pltpu.VMEM((total, nv), BF16),
        pltpu.VMEM((n_plane, share, total), BF16),
        pltpu.VMEM((total, n_q), BF16),
        pltpu.VMEM((half, n_plane, share, n_q), BF16),
        pltpu.VMEM(z_own.shape, F32),
        pltpu.VMEM(z_own.shape, F32),
        pltpu.SemaphoreType.DMA((2,)),
    ]
    args = [place, *pieces, *right, z_own, z_other]
    return kernel_call(body, outs, args, flops, scratch, (len(args) - 2, len(args) - 1))


def in_core_order(own, other, axis):
    first = lax.axis_index("core") == 0
    return jnp.stack([jnp.where(first, own, other), jnp.where(first, other, own)], axis=axis)


def local(amplitudes, grid_factor, metric, virt_energy, pair_energy):
    n_c, n_k, n_d = amplitudes.shape
    _, nv = grid_factor.shape
    n_x, n_h = lax.axis_size("x"), lax.axis_size("y_hi")
    n_z, n_l = lax.axis_size("z"), lax.axis_size("y_lo")
    n_grp = n_z * n_l
    half = n_k // 2
    my_x, my_h, my_core = lax.axis_index("x"), lax.axis_index("y_hi"), lax.axis_index("core")
    my_z, my_l = lax.axis_index("z"), lax.axis_index("y_lo")
    half = n_k // 2
    first = my_core == 0

    other = from_ahead(amplitudes, "core", 1)
    turned = turned_copies(my_core[None], amplitudes, other, n_z * n_l)
    turned = lax.all_to_all(turned, GRP, 0, 0, tiled=True)

    mine = steps_along(grid_factor[None], "y_hi")
    own = [mine] + [from_ahead(mine, "x", o) for o in range(1, n_x)]
    own += [from_ahead(piece, "core", 1) for piece in own]
    columns = placed_by_block(jnp.stack([my_x, my_h, my_core]), own, n_x, n_h).reshape(-1, nv)

    right = right_of(my_core[None], turned, columns, half, FIRST_PART)
    low = from_ahead(right[0], "y_hi", 1)
    high = [right[1]] + [from_ahead(right[1], "x", o) for o in (1, 3, 2)]
    low = jnp.stack([right[0], low])
    high = jnp.stack([high[o] for o in (0, 1, 3, 2)])
    low = {0: low, **{o: from_ahead(low, "x", o) for o in (1, 3, 2)}}
    right = [low[o] for o in range(n_x)] + [high, from_ahead(high, "y_hi", 1)]

    pair = steps_along(grid_factor[None], "y_lo")
    own = {0: pair}
    own[1], own[n_z - 1] = from_ahead(pair, "z", 1), from_ahead(pair, "z", -1)
    own[n_z // 2] = from_ahead(pair, "z", n_z // 2)
    up = from_ahead(jnp.concatenate([pair, own[1]], axis=0), "z", 2)
    down = from_ahead(jnp.concatenate([pair, own[n_z - 1]], axis=0), "z", -2)
    pieces = {(0,): pair, (1,): own[1], (n_z - 1,): own[n_z - 1], (n_z // 2,): own[n_z // 2]}
    order = [*pieces, (2, 3), (n_z - 2, n_z - 3)]
    pieces = {**pieces, order[-2]: up, order[-1]: down}
    others = {}
    for key in order:
        others[key] = from_ahead(pieces[key], "core", 1)
    own = [(key, pieces[key]) for key in order] + [(key, others[key]) for key in order]
    z = metric.reshape(-1, 128)
    z_other = from_ahead(z, "core", 1)
    place = jnp.stack([my_z, my_l, my_x, my_h])
    sums = weighed(place, own, right, z, z_other, half, n_z, n_l, n_x, n_h)
    low, high = sums[:n_x], sums[n_x:]
    high_arrived = to_ahead(high[1], "y_hi", 1)
    low_arrived = [to_ahead(low[o], "x", o) for o in (1, 3, 2)]
    low = [total([low[0][h]] + [p[h] for p in low_arrived]) for h in range(n_h)]
    high = [total([high[0][o], high_arrived[o]]) for o in range(n_x)]
    low_arrived = to_ahead(low[1], "y_hi", 1)
    high_arrived = [to_ahead(high[o], "x", o) for o in (1, 3, 2)]
    parts = [[low[0], low_arrived], [high[0], *high_arrived]]
    ladder = ladder_of(my_core[None], parts, columns, n_grp)
    ladder = lax.all_to_all(ladder, GRP, 0, 0, tiled=True)
    ladder = ladder.astype(F32).sum(axis=0).reshape(n_d, half, 2, n_c)
    keep = jnp.where(first, ladder[:, :, 0], ladder[:, :, 1])
    give = jnp.where(first, ladder[:, :, 1], ladder[:, :, 0])
    other = from_ahead(give.reshape(n_d, half * n_c), "core", 1).reshape(n_d, half, n_c)
    ladder = in_core_order(keep, other, 1).reshape(n_d, n_k, n_c).transpose(2, 1, 0)
    first_energy = lax.dynamic_slice_in_dim(virt_energy, lax.axis_index(BLK) * n_c, n_c)
    second_energy = lax.dynamic_slice_in_dim(virt_energy, lax.axis_index(GRP) * n_d, n_d)
    denominator = (
        first_energy[:, None, None] + second_energy[None, None, :] - pair_energy[None, :, None]
    )
    return denominator * amplitudes.astype(F32) + ladder


def solution(mesh):
    split = Mesh(mesh.devices.reshape(4, 2, 2, 2, 8), ("x", "y_hi", "core", "y_lo", "z"))
    in_specs = (P(BLK, None, GRP), P(BLK + GRP, None), P(BLK, GRP, None), P(), P())
    return jax.shard_map(
        local, mesh=split, in_specs=in_specs, out_specs=P(BLK, None, GRP), check_vma=False
    )
```
